512 devices in a mesh: grp: 2 (over y), dp: 256 (over z, x, core).
Axes of the slice: x: 8, y: 2, z: 16, core: 2. Of those that a mesh axis runs over, the one named last changes fastest.
The devices are a block of a 8x8x16 slice.
Arguments:
- params: float32 [1900544], P(('grp', 'dp')), parts along dimension 0, may hold values from -0.3 to 0.3
- momentum: float32 [1900544], P(('grp', 'dp')), parts along dimension 0, may hold values from -6 to 6
- noise_draws: float32 [2, 950272], P('grp', 'dp'), parts along dimension 0, may hold values from -6 to 6
- images: float32 [262144, 448], P(('grp', 'dp')), parts along dimension 0, may hold values from -6 to 6
- labels: int32 [262144], P(('grp', 'dp')), parts along dimension 0, may hold values from 0 to 9
- indices: int32 [2, 65536], P('grp', 'dp'), parts along dimension 0, may hold values from 0 to 511
Outputs:
- params_out: float32 [1900544], P(('grp', 'dp')), parts along dimension 0
- momentum_out: float32 [1900544], P(('grp', 'dp')), parts along dimension 0
- losses: float32 [2], P('grp'), parts along dimension 0
The draws below stay inside these ranges and needn't reach their ends.
There are 2 independent parts, one for each index of `grp`. The reference program is written for one: setup_inputs(seed, part) draws one part's arguments, and reference() takes and returns one part's arrays. A program takes and returns all parts, laid end to end along the dimension named above; each array names one. Nothing has to cross between parts.
All inputs are finite; a program needn't handle non-finite values.
Results may differ from the reference program's by a relative error of at most 0.0003.
Values sent between devices are 32-bit elements; how exact they have to be, the bound alone decides.
A program may use at most 64 MiB of HBM per device.

```python
import math
import jax
import jax.numpy as jnp
from jax import lax

DIN = 448
H = 2048
OUT = 10
POOL_DEV = 512
BATCH_DEV = 256
STEPS = 1
PARAMS = 950272
POOL = 131072
BATCH = 65536
N_DP = 256


def place_ends(drawn, own_key, least, high):
    extent = drawn.shape
    spot = [jax.random.randint(jax.random.fold_in(own_key, axis), (), 0, extent[axis]) for axis in range(len(extent))]
    drawn = drawn.at[tuple(spot)].set(least)
    longest = extent.index(max(extent))
    spot[longest] = (spot[longest] + 1) % extent[longest]
    return drawn.at[tuple(spot)].set(high)


def shard_levels(key, extent, pieces, least, largest):
    def one(axis_at, parts):
        steps = jax.random.uniform(jax.random.fold_in(jax.random.fold_in(key, 6), axis_at), (parts,), jnp.float32, least / len(pieces), largest / len(pieces))
        return jnp.repeat(jnp.exp(steps), extent[axis_at] // parts).reshape((-1,) + (1,) * (len(extent) - axis_at - 1))

    level = one(*pieces[0])
    for cut in pieces[1:]:
        level = level * one(*cut)
    return level


def centred(key, extent, scale, bound, shards=(), kind=jnp.bfloat16):
    values = jax.random.normal(key, extent, jnp.float32) * scale
    if len(shards) > 0:
        values = shard_levels(key, extent, shards, -0.22, 0.18) * values
    return jnp.clip(values, min=-bound, max=bound).astype(kind)


def setup_inputs(seed: int = 0, part: int = 0) -> dict:
    seeds = jax.random.split(jax.random.key(seed), 7)
    own_keys = jax.random.split(jax.random.fold_in(seeds[6], part), 7)
    params = centred(own_keys[0], (PARAMS,), 0.05, 0.3, ((0, 256),), jnp.float32)
    momentum = centred(own_keys[1], (PARAMS,), 1.0, 6.0, ((0, 256),), jnp.float32)
    noise_draws = centred(own_keys[2], (STEPS, PARAMS), 1.0, 6.0, ((1, 256),), jnp.float32)
    images = centred(own_keys[3], (POOL, DIN), 1.0, 6.0, ((0, 256),), jnp.float32)
    labels = place_ends(jax.random.randint(own_keys[4], (POOL,), 0, OUT), jax.random.fold_in(own_keys[4], 1), 0, OUT - 1).astype(jnp.int32)
    indices = place_ends(jax.random.randint(own_keys[5], (STEPS, BATCH), 0, POOL_DEV), jax.random.fold_in(own_keys[5], 1), 0, POOL_DEV - 1).astype(jnp.int32)
    return {"params": params, "momentum": momentum, "noise_draws": noise_draws, "images": images, "labels": labels, "indices": indices}


step_size = 0.02
friction = 15.0

def unpack(flat_vec):
    in_end = DIN * H
    w_in = flat_vec[:in_end].reshape(DIN, H)
    b_in = flat_vec[in_end:in_end + H]
    hid_end = in_end + H
    w_out = flat_vec[hid_end:hid_end + H * OUT].reshape(H, OUT)
    b_out = flat_vec[hid_end + H * OUT:hid_end + H * OUT + OUT]
    return (w_in, b_in, w_out, b_out)

def total_nll(flat_vec, chosen_rows, targets):
    w_in, b_in, w_out, b_out = unpack(flat_vec)
    hidden = jnp.tanh(jnp.dot(chosen_rows, w_in, precision=lax.Precision.HIGHEST, preferred_element_type=jnp.float32) + b_in)
    logits = jnp.dot(hidden, w_out, precision=lax.Precision.HIGHEST, preferred_element_type=jnp.float32) + b_out
    log_norm = jnp.log(lax.optimization_barrier(jnp.sum(jnp.exp(logits), axis=1)))
    classes = lax.broadcasted_iota(jnp.int32, logits.shape, 1)
    picked = lax.optimization_barrier(jnp.sum(jnp.where(targets[:, None] == classes, logits, 0.0), axis=1))
    return jnp.sum(log_norm - picked)

def prior_precision(flat_index):
    in_end = DIN * H
    hid_end = in_end + H
    out_end = hid_end + H * OUT
    return jnp.where(flat_index < in_end, float(DIN), jnp.where(flat_index < hid_end, 1.0, jnp.where(flat_index < out_end, float(H), 1.0)))

def reference(params, momentum, noise_draws, images, labels, indices):
    offsets = jnp.arange(BATCH, dtype=jnp.int32) // BATCH_DEV * POOL_DEV
    precision = prior_precision(jnp.arange(PARAMS, dtype=jnp.int32))
    losses = []
    for step_idx in range(STEPS):
        pool_rows = (indices[step_idx].astype(jnp.int32) + offsets).astype(jnp.int32)
        blocks = pool_rows.reshape(N_DP, BATCH_DEV)

        def one_block(carry, block):
            chosen_rows = images[block]
            targets = labels[block]
            nll_part, pullback = jax.vjp(lambda weights_flat: total_nll(weights_flat, chosen_rows, targets), params)
            local_grad, = pullback(jnp.ones_like(nll_part))
            return ((carry[0] + local_grad, carry[1] + nll_part), None)
        start_carry = (jnp.zeros((PARAMS,), jnp.float32), jnp.zeros((), jnp.float32))
        (grad_sum, nll_sum), _ = lax.scan(one_block, start_carry, blocks)
        losses.append(nll_sum / BATCH)
        total_force = POOL / BATCH * grad_sum + precision * params
        momentum = (1.0 - step_size * friction) * momentum - step_size * total_force + math.sqrt(2.0 * friction * step_size) * noise_draws[step_idx]
        params = params + step_size * momentum
    return (params, momentum, jnp.stack(losses))
```

```python
import functools
import math

import jax
import jax.numpy as jnp
from jax import lax
from jax.experimental import pallas as pl
from jax.experimental.pallas import tpu as pltpu
from jax.sharding import Mesh
from jax.sharding import PartitionSpec as P

DIN = 448
H = 2048
OUT = 10
NZ, NX, NC = 16, 8, 2
LANES = 128
ROW = H // LANES
HALF = ROW // 2
HID = H // 2
ZROWS = 29
ZPAD = 32
BLK = ZPAD * HALF
SUB0 = 15 * HALF
KPAD = 16
W2L = HID * OUT // LANES
DP = ("dp_0", "dp_1", "dp_2")
GRP_DP = ("grp", "dp_0", "dp_1", "dp_2")
MESH = pl.DeviceIdType.MESH
F32 = jnp.float32
BF16 = jnp.bfloat16

step_size = 0.02
friction = 15.0


def split(value):
    high = value.astype(BF16)
    return high, (value - high.astype(F32)).astype(BF16)


def dot(a, b):
    return jnp.dot(a, b, preferred_element_type=F32)


def dot_nt(a, b):
    return lax.dot_general(a, b, (((1,), (1,)), ((), ())), preferred_element_type=F32)


def iota(shape, dim):
    return lax.broadcasted_iota(jnp.int32, shape, dim)


def tenth(e):
    return (e * 6554) >> 16


def kernel(
    nz, nx, slot, lines, tail_z, tail_r,
    par, idx, lab, img_any, out,
    img, xs, ys, xh, xl, xth, xtl, slots, zrow, gh, tp, tt, hidf, hidh, hidl, lg, w48, dl48, dwl, ep, ee,
    d2, rb, pk, sx, rx,
    img_sem, dd_send, dd_recv, xs_send, xf_send, xs_recv, zs_send, zs_recv, rs_send, rs_recv, rx_send, rx_recv,
):
    batch = idx.shape[1]
    pool = lab.shape[1]
    din = img.shape[1]
    kdim = nz * ZPAD
    g, z, x, c = (lax.axis_index(a) for a in GRP_DP)
    oc = 1 - c
    partner = (g, z, x, oc)
    zside = ((g, lax.rem(z + 1, nz), x, c), (g, lax.rem(z + nz - 1, nz), x, c))
    half_nz = nz // 2

    def zmod(v):
        return lax.rem(v + 2 * nz, nz)

    def xpos(dx):
        return lax.rem(x + dx, nx)

    deltas = []
    for d in range(1, nx // 2 + 1):
        for v in (d, nx - d):
            if v not in deltas:
                deltas.append(v)

    image_copy = pltpu.make_async_copy(img_any, img, img_sem)
    image_copy.start()

    barrier = pltpu.get_barrier_semaphore()
    peers = [partner, zside[0], zside[1]] + [(g, z, xpos(d), c) for d in deltas]
    for peer in peers:
        pl.semaphore_signal(barrier, inc=1, device_id=peer, device_id_type=MESH)

    zeros_pad = jnp.zeros((BLK - ZROWS * HALF, LANES), F32)
    for zz in range(nz):
        gh[zz * BLK + ZROWS * HALF : (zz + 1) * BLK, :] = zeros_pad

    def remote(src, dst, send, recv, to):
        return pltpu.make_async_remote_copy(
            src_ref=src, dst_ref=dst, send_sem=send, recv_sem=recv, device_id=to, device_id_type=MESH
        )

    def at(ref, start, size, step=8):
        return ref.at[pl.ds(pl.multiple_of(start, step), size)]

    pl.semaphore_wait(barrier, len(peers))

    mine = 2 * x + c

    def place(k):
        return at(slots, k * slot, slot)

    x_sends = []
    for i, d in enumerate(deltas):
        x_sends.append(remote(par, place(mine), xs_send.at[i], xs_recv.at[mine], (g, z, xpos(d), c)))
    x_sends.append(remote(par, place(mine), xs_send.at[nx - 1], xs_recv.at[mine], partner))
    for copy in x_sends:
        copy.start()
    slots[pl.ds(pl.multiple_of(mine * slot, 8), slot), :] = par[...]

    image_copy.wait()
    hot_t = (iota((pool, batch), 0) == idx[...]).astype(F32)
    hot = hot_t.T.astype(BF16)
    q = iota((din, kdim), 1)
    spread = ((q & (ZPAD - 1)) < ZROWS) & (iota((din, kdim), 0) == (q >> 5) * ZROWS + (q & (ZPAD - 1)))
    spread = spread.astype(F32).astype(BF16)
    img_h, img_l = split(img[...])
    rows = dot(dot(hot, img_h).astype(BF16), spread) + dot(dot(hot, img_l).astype(BF16), spread)
    rows = rows + (iota((batch, kdim), 1) == tail_z * ZPAD + tail_r).astype(F32)
    xs[pl.ds(pl.multiple_of(c * batch, 8), batch), :] = rows
    lab_hot = (iota((KPAD, pool), 0) == lab[...]).astype(F32).astype(BF16)
    ys[pl.ds(pl.multiple_of(c * KPAD, 8), KPAD), :] = dot(lab_hot, hot_t.astype(BF16))
    row_copy = remote(at(xs, c * batch, batch), at(xs, c * batch, batch), dd_send.at[0], dd_recv.at[0], partner)
    hot_copy = remote(at(ys, c * KPAD, KPAD), at(ys, c * KPAD, KPAD), dd_send.at[1], dd_recv.at[1], partner)

    def arrived(k, i, to):
        return remote(place(k), place(k), xf_send.at[i], xs_recv.at[k], to)

    forwards = []
    for i, d in enumerate(deltas):
        k = 2 * xpos(d) + c
        copy = arrived(k, i, partner)
        copy.wait_recv()
        copy.start()
        forwards.append(copy)
    row_copy.start()
    hot_copy.start()
    for i, d in enumerate([0] + deltas):
        k = 2 * xpos(d) + oc
        arrived(k, 0, partner).wait_recv()
    for k in range(2 * nx):
        zrow[lines * k : lines * (k + 1), :] = slots[slot * k : slot * k + lines, :]
    for r in range(ZROWS):
        gh[pl.ds(pl.multiple_of(z * BLK + HALF * r, 8), HALF), :] = zrow[
            pl.ds(pl.multiple_of(ROW * r + HALF * c, 8), HALF), :
        ]

    sub_size = (SUB0, ZROWS * HALF - SUB0)

    def ag(way, hop, sub, back):
        sign = 1 if way == 0 else -1
        block = zmod(z - sign * (hop - 1 + back))
        ref = at(gh, block * BLK + sub * SUB0, sub_size[sub])
        return remote(ref, ref, zs_send.at[way, hop - 1, sub], zs_recv.at[way, hop - 1, sub], zside[way])

    def each(fn):
        for sub in range(2):
            for way in range(2):
                fn(way, sub)

    each(lambda way, sub: ag(way, 1, sub, 0).start())

    row_copy.wait_recv()
    hot_copy.wait_recv()
    for part in range(2 * batch // 128):
        span = slice(128 * part, 128 * (part + 1))
        value = xs[span, :]
        xh[span, :], xl[span, :] = split(value)
        xth[:, span], xtl[:, span] = split(value.T)

    def ag_hop(hop, _):
        def one(way, sub):
            ag(way, hop - 1, sub, 1).wait_recv()
            ag(way, hop, sub, 0).start()

        each(one)
        return 0

    lax.fori_loop(2, half_nz, ag_hop, 0)
    each(lambda way, sub: ag(way, half_nz - 1, sub, 1).wait_recv())
    for way in range(2):
        ag(way, half_nz, way, 0).start()
    for way in range(2):
        ag(way, half_nz, way, 1).wait_recv()

    tail = tail_z * BLK + tail_r * HALF
    tail_copy = remote(gh.at[tail : tail + 12 * HALF], tp, dd_send.at[2], dd_recv.at[2], partner)
    tail_copy.start()

    def forward(n, _):
        w = jnp.concatenate(
            [gh[pl.ds(2 * n, kdim, stride=HALF), :], gh[pl.ds(2 * n + 1, kdim, stride=HALF), :]], axis=1
        )
        wh, wl = split(w)
        pre = dot(xh[...], wh) + dot(xh[...], wl) + dot(xl[...], wh)
        hid = jnp.tanh(pre)
        span = pl.ds(pl.multiple_of(256 * n, 256), 256)
        hidf[:, span] = hid
        hidh[:, span], hidl[:, span] = split(hid)
        return 0

    lax.fori_loop(0, HID // 256, forward, 0)

    tail_copy.wait_recv()
    for r in range(12):
        tt[pl.ds(pl.multiple_of(ROW * r + HALF * c, 8), HALF), :] = gh[tail + HALF * r : tail + HALF * (r + 1), :]
        tt[pl.ds(pl.multiple_of(ROW * r + HALF * oc, 8), HALF), :] = tp[HALF * r : HALF * (r + 1), :]
    dwl[...] = tt[pl.ds(pl.multiple_of(ROW + W2L * c, 8), W2L), :]
    groups = HID // LANES
    pieces = []
    for i in range(OUT):
        e = iota((KPAD, LANES), 1) + LANES * i
        keep = (e - OUT * tenth(e)) == iota((KPAD, LANES), 0)
        line = dwl[pl.ds(i, groups, stride=OUT), :]
        spread_line = jnp.where(keep[None], line[:, None, :], 0.0)
        pieces.append(spread_line.reshape(groups * KPAD, LANES))
    wide_h, wide_l = split(jnp.concatenate(pieces, axis=1))
    pick = (tenth(iota((OUT * LANES, LANES), 0)) == iota((OUT * LANES, LANES), 1)).astype(F32).astype(BF16)
    w2b = dot(wide_h, pick) + dot(wide_l, pick)
    w2t = jnp.concatenate([w2b[KPAD * m : KPAD * (m + 1), :] for m in range(groups)], axis=1)
    w2h, w2l = split(w2t)
    w48[...] = jnp.concatenate([w2h, w2l, w2h], axis=0)
    both = dot_nt(w48[0 : 2 * KPAD, :], hidh[...])
    part_logits = both[:KPAD] + both[KPAD:] + dot_nt(w48[0:KPAD, :], hidl[...])
    lg[pl.ds(pl.multiple_of(c * KPAD, 8), KPAD), :] = part_logits
    logit_copy = remote(at(lg, c * KPAD, KPAD), at(lg, c * KPAD, KPAD), dd_send.at[3], dd_recv.at[3], partner)
    logit_copy.start()
    b2_line = tt[ROW + 2 * W2L : ROW + 2 * W2L + 1, :]
    b2 = jnp.sum(jnp.where(iota((KPAD, LANES), 0) == iota((KPAD, LANES), 1), b2_line, 0.0), axis=1, keepdims=True)
    real = iota((KPAD, 2 * batch), 0) < OUT
    b2 = jnp.where(iota((KPAD, 1), 0) < OUT, b2, 0.0)
    targets = jnp.concatenate([ys[0:KPAD, :], ys[KPAD : 2 * KPAD, :]], axis=1)
    logit_copy.wait_recv()
    logits = lg[0:KPAD, :] + lg[KPAD : 2 * KPAD, :] + b2
    expo = jnp.where(real, jnp.exp(logits), 0.0)
    norm = jnp.sum(expo, axis=0, keepdims=True)
    picked = jnp.sum(targets * logits, axis=0, keepdims=True)
    nll = jnp.sum(jnp.log(norm) - picked, axis=1, keepdims=True)
    dlog = expo / norm - targets
    dlh, dll = split(dlog)
    dl3 = jnp.concatenate([dlh.astype(F32), dlh.astype(F32), dll.astype(F32)], axis=0)
    dl48[...] = dl3.T.astype(BF16)

    dlhl = jnp.concatenate([dlh, dll], axis=0)
    both = dot(dlhl, hidh[...])
    dw2t = both[:KPAD] + both[KPAD:] + dot(dlh, hidl[...])
    dw2b = jnp.concatenate([dw2t[:, LANES * m : LANES * (m + 1)] for m in range(groups)], axis=0)
    dwh, dwlo = split(dw2b)
    e = iota((LANES, OUT * LANES), 1)
    place_back = (tenth(e) == iota((LANES, OUT * LANES), 0)).astype(F32).astype(BF16)
    flat = dot(dwh, place_back) + dot(dwlo, place_back)
    e = iota((groups * KPAD, OUT * LANES), 1)
    flat = jnp.where((e - OUT * tenth(e)) == (iota((groups * KPAD, OUT * LANES), 0) & (KPAD - 1)), flat, 0.0)
    flat = jnp.sum(flat.reshape(groups, KPAD, OUT * LANES), axis=1)
    for i in range(OUT):
        dwl[pl.ds(i, groups, stride=OUT), :] = flat[:, LANES * i : LANES * (i + 1)]
    grad_copy = remote(dwl, ep, dd_send.at[4], dd_recv.at[4], partner)
    grad_copy.start()
    ee[2 * W2L : 2 * W2L + ROW, :] = jnp.zeros((ROW, LANES), F32)
    db2 = jnp.sum(dlog, axis=1, keepdims=True)
    ee[2 * W2L : 2 * W2L + 1, :] = jnp.sum(
        jnp.where(iota((KPAD, LANES), 0) == iota((KPAD, LANES), 1), db2, 0.0), axis=0, keepdims=True
    )
    ee[pl.ds(pl.multiple_of(W2L * c, 8), W2L), :] = dwl[...]

    def backward(n, _):
        span = pl.ds(pl.multiple_of(256 * n, 256), 256)
        h = hidf[:, span]
        dh, dl = split(dot(dl48[...], w48[:, span]) * (1.0 - h * h))
        grad = dot(xth[...], dh) + dot(xth[...], dl) + dot(xtl[...], dh)
        d2[pl.ds(2 * n, kdim, stride=HALF), :] = grad[:, :LANES]
        d2[pl.ds(2 * n + 1, kdim, stride=HALF), :] = grad[:, LANES:]
        return 0

    lax.fori_loop(0, HID // 256, backward, 0)
    nll_lines = jnp.broadcast_to(nll, (HALF, LANES))
    for zz in range(nz):
        d2[zz * BLK + ZROWS * HALF : zz * BLK + (ZROWS + 1) * HALF, :] = nll_lines
    grad_copy.wait_recv()
    ee[pl.ds(pl.multiple_of(W2L * oc, 8), W2L), :] = ep[...]
    for r in range(11):
        d2[tail + HALF * (r + 1) : tail + HALF * (r + 2), :] = ee[pl.ds(pl.multiple_of(ROW * r + HALF * c, 8), HALF), :]

    def rs(way, hop, sub, back):
        sign = 1 if way == 0 else -1
        block = zmod(z + sign * (half_nz + 1 - hop - back))
        src = at(d2, block * BLK + sub * SUB0, SUB0)
        dst = at(rb, ((way * half_nz + hop - 1) * 2 + sub) * SUB0, SUB0)
        return remote(src, dst, rs_send.at[way, hop - 1, sub], rs_recv.at[way, hop - 1, sub], zside[way])

    def add_arrived(way, hop, sub):
        sign = 1 if way == 0 else -1
        rs(way, hop, sub, 0).wait_recv()
        block = zmod(z + sign * (half_nz - hop))
        span = pl.ds(pl.multiple_of(block * BLK + sub * SUB0, 8), SUB0)
        got = pl.ds(pl.multiple_of(((way * half_nz + hop - 1) * 2 + sub) * SUB0, 8), SUB0)
        d2[span, :] = d2[span, :] + rb[got, :]

    for way in range(2):
        rs(way, 1, way, 0).start()
    for way in range(2):
        rs(way, 2, 1 - way, 0).start()
    for way in range(2):
        add_arrived(way, 1, way)
        rs(way, 2, way, 0).start()

    def rs_hop(hop, _):
        def one(way, sub):
            add_arrived(way, hop - 1, sub)
            rs(way, hop, sub, 0).start()

        each(one)
        return 0

    lax.fori_loop(3, half_nz + 1, rs_hop, 0)
    each(lambda way, sub: add_arrived(way, half_nz, sub))

    own = at(d2, z * BLK, 2 * SUB0)
    swap = remote(own, pk, dd_send.at[5], dd_recv.at[5], partner)
    swap.start()
    for r in range(ZROWS):
        zrow[pl.ds(pl.multiple_of(ROW * r + HALF * c, 8), HALF), :] = d2[
            pl.ds(pl.multiple_of(z * BLK + HALF * r, 8), HALF), :
        ]
    loss_line = d2[pl.ds(pl.multiple_of(z * BLK + HALF * ZROWS, 8), 8), :]
    swap.wait_recv()
    for r in range(ZROWS):
        zrow[pl.ds(pl.multiple_of(ROW * r + HALF * oc, 8), HALF), :] = pk[HALF * r : HALF * (r + 1), :]
    for core in range(2):

        @pl.when(c == core)
        def _():
            for k in range(nx):
                first = lines * (2 * k + core)
                sx[slot * k : slot * k + lines, :] = zrow[first : first + lines, :]
                sx[slot * k + lines : slot * k + lines + 1, :] = loss_line[0:1, :]

    finals = []
    for i, d in enumerate(deltas):
        to = xpos(d)
        finals.append(
            remote(at(sx, to * slot, slot), at(rx, x * slot, slot), rx_send.at[i], rx_recv.at[x], (g, z, to, c))
        )
    for copy in finals:
        copy.start()
    total = sx[pl.ds(pl.multiple_of(x * slot, 8), slot), :]
    for i, d in enumerate(deltas):
        source = xpos(d)
        remote(at(sx, source * slot, slot), at(rx, source * slot, slot), rx_send.at[i], rx_recv.at[source], partner).wait_recv()
        total = total + rx[pl.ds(pl.multiple_of(source * slot, 8), slot), :]
    out[...] = total

    for copy in x_sends + forwards + [row_copy, hot_copy, tail_copy, logit_copy, grad_copy, swap] + finals:
        copy.wait_send()

    def drain(hop, _):
        each(lambda way, sub: ag(way, hop, sub, 0).wait_send())
        each(lambda way, sub: rs(way, hop + 1, sub, 0).wait_send())
        return 0

    lax.fori_loop(1, half_nz, drain, 0)
    for way in range(2):
        ag(way, half_nz, way, 0).wait_send()
        rs(way, 1, way, 0).wait_send()


def summed_gradient(shard, picked, labels, images, nz, nx):
    lines = shard.shape[0] // LANES
    slot = -(-(lines + 1) // 8) * 8
    batch, pool, din = picked.shape[1], images.shape[0], images.shape[1]
    kdim = nz * ZPAD
    half_nz = nz // 2
    padded = jnp.pad(shard, (0, slot * LANES - shard.shape[0])).reshape(slot, LANES)
    vmem = pl.BlockSpec(memory_space=pltpu.VMEM)
    dma = pltpu.SemaphoreType.DMA
    tail_z, tail_r = divmod(din, ZROWS)
    return pl.pallas_call(
        functools.partial(kernel, nz, nx, slot, lines, tail_z, tail_r),
        out_shape=jax.ShapeDtypeStruct((slot, LANES), F32),
        in_specs=[vmem, vmem, vmem, pl.BlockSpec(memory_space=pl.ANY)],
        out_specs=vmem,
        scratch_shapes=[
            pltpu.VMEM((pool, din), F32),
            pltpu.VMEM((2 * batch, kdim), F32),
            pltpu.VMEM((2 * KPAD, batch), F32),
            pltpu.VMEM((2 * batch, kdim), BF16),
            pltpu.VMEM((2 * batch, kdim), BF16),
            pltpu.VMEM((kdim, 2 * batch), BF16),
            pltpu.VMEM((kdim, 2 * batch), BF16),
            pltpu.VMEM((2 * nx * slot, LANES), F32),
            pltpu.VMEM((ZROWS * ROW, LANES), F32),
            pltpu.VMEM((nz * BLK, LANES), F32),
            pltpu.VMEM((12 * HALF, LANES), F32),
            pltpu.VMEM((12 * ROW, LANES), F32),
            pltpu.VMEM((2 * batch, HID), F32),
            pltpu.VMEM((2 * batch, HID), BF16),
            pltpu.VMEM((2 * batch, HID), BF16),
            pltpu.VMEM((2 * KPAD, 2 * batch), F32),
            pltpu.VMEM((3 * KPAD, HID), BF16),
            pltpu.VMEM((2 * batch, 3 * KPAD), BF16),
            pltpu.VMEM((W2L, LANES), F32),
            pltpu.VMEM((W2L, LANES), F32),
            pltpu.VMEM((2 * W2L + ROW, LANES), F32),
            pltpu.VMEM((nz * BLK, LANES), F32),
            pltpu.VMEM((2 * half_nz * 2 * SUB0, LANES), F32),
            pltpu.VMEM((2 * SUB0, LANES), F32),
            pltpu.VMEM((nx * slot, LANES), F32),
            pltpu.VMEM((nx * slot, LANES), F32),
            dma,
            dma((6,)),
            dma((6,)),
            dma((nx,)),
            dma((nx,)),
            dma((2 * nx,)),
            dma((2, half_nz, 2)),
            dma((2, half_nz, 2)),
            dma((2, half_nz, 2)),
            dma((2, half_nz, 2)),
            dma((nx,)),
            dma((nx,)),
        ],
        compiler_params=pltpu.CompilerParams(
            collective_id=0, has_side_effects=True, vmem_limit_bytes=56 * 1024 * 1024
        ),
    )(padded, picked, labels.reshape(1, -1), images)


def prior_precision(flat_index):
    in_end = DIN * H
    hid_end = in_end + H
    out_end = hid_end + H * OUT
    return jnp.where(
        flat_index < in_end,
        float(DIN),
        jnp.where(flat_index < hid_end, 1.0, jnp.where(flat_index < out_end, float(H), 1.0)),
    )


def body(params, momentum, noise_draws, images, labels, indices):
    shard_len = params.shape[0]
    shard_start = lax.axis_index(DP) * shard_len
    precision = prior_precision(shard_start + lax.iota(jnp.int32, shard_len))
    scale_data = images.shape[0] / indices.shape[1]
    row_count = lax.axis_size(DP) * indices.shape[1]
    summed = summed_gradient(params, indices, labels, images, lax.axis_size("dp_0"), lax.axis_size("dp_1"))
    lines = shard_len // LANES
    own_grad = summed[:lines].reshape(shard_len)
    losses = summed[lines, 0:1] / row_count
    total_force = scale_data * own_grad + precision * params
    momentum = (
        (1.0 - step_size * friction) * momentum
        - step_size * total_force
        + math.sqrt(2.0 * friction * step_size) * noise_draws[0]
    )
    params = params + step_size * momentum
    return (params, momentum, losses)


def solution(mesh):
    torus = Mesh(mesh.devices.reshape(mesh.shape["grp"], NZ, NX, NC), GRP_DP)
    placed = (P(GRP_DP), P(GRP_DP), P("grp", DP), P(GRP_DP, None), P(GRP_DP), P("grp", DP))
    return jax.shard_map(
        body,
        mesh=torus,
        in_specs=placed,
        out_specs=(P(GRP_DP), P(GRP_DP), P("grp")),
        check_vma=False,
    )
```
